64 devices in a mesh: dp: 8 (over x, y, core), tp: 8 (over z).
Axes of the slice: x: 2, y: 2, z: 8, core: 2. Of those that a mesh axis runs over, the one named last changes fastest.
The devices are a block of a 4x4x8 slice.
Arguments:
- x: bfloat16 [16384, 2304], P('dp'), parts along dimension 0
- dy: bfloat16 [16384, 2304], P('dp'), parts along dimension 0
- gate: bfloat16 [16384, 9216], P('dp', 'tp'), parts along dimension 0
- up: bfloat16 [16384, 9216], P('dp', 'tp'), parts along dimension 0
- w_gate: bfloat16 [2304, 9216], P(None, 'tp')
- w_up: bfloat16 [2304, 9216], P(None, 'tp')
- w_down: bfloat16 [9216, 2304], P('tp')
Outputs:
- output 1: bfloat16 [16384, 2304], P('dp'), parts along dimension 0
- output 2: bfloat16 [18432, 9216], P('dp', 'tp'), parts along dimension 0
- output 3: bfloat16 [18432, 9216], P('dp', 'tp'), parts along dimension 0
- output 4: bfloat16 [73728, 2304], P(('dp', 'tp')), parts along dimension 0
There are 8 independent parts. The reference program is written for one: setup_inputs(seed, part) draws one part's arguments, and reference() takes and returns one part's arrays. A program takes and returns all parts, laid end to end along the dimension named above; an argument that names none is the same for every part.
All inputs are finite; a program needn't handle non-finite values.
Results may differ from the reference program's by a relative error of at most 0.012.
Values are sent between devices in bfloat16 or wider.
A program may use at most 768 MiB of HBM per device.

```python
import jax
import jax.numpy as jnp

ROWS = 2048
D = 2304
FF = 9216


def act(gate, up):
    return jax.nn.gelu(gate) * up


def setup_inputs(seed: int = 0, part: int = 0) -> dict:
    kx, ky, ka, kb, kg, ku, kd = jax.random.split(jax.random.key(seed), 7)
    kx, ky, ka, kb = (jax.random.fold_in(k, part) for k in (kx, ky, ka, kb))
    drawn = {
        "x": jax.random.normal(kx, (ROWS, D), jnp.float32),
        "dy": jax.random.normal(ky, (ROWS, D), jnp.float32),
        "gate": jax.random.normal(ka, (ROWS, FF), jnp.float32),
        "up": jax.random.normal(kb, (ROWS, FF), jnp.float32),
        "w_gate": jax.random.normal(kg, (D, FF), jnp.float32) * D**-0.5,
        "w_up": jax.random.normal(ku, (D, FF), jnp.float32) * D**-0.5,
        "w_down": jax.random.normal(kd, (FF, D), jnp.float32) * FF**-0.5,
    }
    return {k: v.astype(jnp.bfloat16) for k, v in drawn.items()}


def reference(x, dy, gate, up, w_gate, w_up, w_down):
    hidden, back = jax.vjp(act, gate.astype(jnp.float32), up.astype(jnp.float32))
    d_hidden = jnp.dot(dy, w_down.T, preferred_element_type=jnp.float32)
    d_gate, d_up = (g.astype(jnp.bfloat16) for g in back(d_hidden))
    dx = jnp.dot(d_gate, w_gate.T, preferred_element_type=jnp.float32) + jnp.dot(d_up, w_up.T, preferred_element_type=jnp.float32)
    dw_gate = jnp.dot(x.T, d_gate, preferred_element_type=jnp.float32)
    dw_up = jnp.dot(x.T, d_up, preferred_element_type=jnp.float32)
    dw_down = jnp.dot(hidden.astype(jnp.bfloat16).T, dy, preferred_element_type=jnp.float32)
    return tuple(g.astype(jnp.bfloat16) for g in (dx, dw_gate, dw_up, dw_down))
```

```python
import functools

import jax
import jax.numpy as jnp
from jax import lax
from jax.experimental import pallas as pl
from jax.experimental.pallas import tpu as pltpu
from jax.sharding import PartitionSpec as P

MESH = pl.DeviceIdType.MESH
F32 = jnp.float32
BF16 = jnp.bfloat16
PIECES = 3
TILE = 384


def act(gate, up):
    return jax.nn.gelu(gate) * up


def dot_nt(a, b):
    return lax.dot_general(a, b, (((1,), (1,)), ((), ())), preferred_element_type=F32)


def dot_tn(a, b):
    return lax.dot_general(a, b, (((0,), (0,)), ((), ())), preferred_element_type=F32)


def kernel(
    n,
    x, dy, gate, up, w_gate, w_up, w_down,
    dx, dw_gate, dw_up, dw_down,
    w_gu, w_d, d_gu, hid, dy_v, term, slots, stage,
    row_sem, wd_sem, wgu_sem, x_sem, out_sem, own_sem, rs_send, rs_recv, ag_send, ag_recv,
):
    tokens, width = dy_v.shape
    ff = w_d.shape[0]
    block = tokens // n
    half = block // 2
    piece = width // PIECES
    ff_piece = ff // PIECES
    me = lax.axis_index("tp")
    right, left = lax.rem(me + 1, n), lax.rem(me + n - 1, n)
    peers = (right, left)

    def rows_of(side, step):
        if side == 0:
            return pl.ds(pl.multiple_of(lax.rem(me - step + 2 * n, n) * block, block), half)
        return pl.ds(pl.multiple_of(lax.rem(me + step + n, n) * block + half, half), half)

    def held(side, step):
        return pl.ds(pl.multiple_of(step * block + side * half, half), half)

    def row_loads(step):
        parity = lax.rem(step, 2)
        copies = []
        for side in range(2):
            src, dst = rows_of(side, step), held(side, step)
            pairs = (
                (dy.at[src, :], dy_v.at[dst, :]),
                (gate.at[src, :], d_gu.at[dst, pl.ds(0, ff)]),
                (up.at[src, :], d_gu.at[dst, pl.ds(ff, ff)]),
            )
            for i, (a, b) in enumerate(pairs):
                copies.append(pltpu.make_async_copy(a, b, row_sem.at[parity, side * 3 + i]))
        return copies

    def wd_load(i):
        rows = pl.ds(i * ff_piece, ff_piece)
        return pltpu.make_async_copy(w_down.at[rows, :], w_d.at[rows, :], wd_sem.at[i])

    def wgu_loads(i):
        rows = pl.ds(i * piece, piece)
        return [
            pltpu.make_async_copy(w.at[rows, :], w_gu.at[rows, pl.ds(j * ff, ff)], wgu_sem.at[i, j])
            for j, w in enumerate((w_gate, w_up))
        ]

    def x_load(side, step):
        return pltpu.make_async_copy(x.at[rows_of(side, step), :], w_gu.at[held(side, step), :], x_sem.at[step, side])

    def rs_copy(side, step, c):
        return pltpu.make_async_remote_copy(
            src_ref=slots.at[side, step, c],
            dst_ref=slots.at[side, step + 1, c],
            send_sem=rs_send.at[side, step, c],
            recv_sem=rs_recv.at[side, step + 1, c],
            device_id={"tp": peers[side]},
            device_id_type=MESH,
        )

    def columns(c):
        return pl.ds(pl.multiple_of(c * piece, piece), piece)

    def ag_rows(side, hop):
        return rows_of(side, hop + n - 1)

    def ag_copy(side, hop, c, first):
        place = dx.at[ag_rows(side, hop), columns(c)]
        return pltpu.make_async_remote_copy(
            src_ref=slots.at[side, n - 1, c] if first else place,
            dst_ref=place,
            send_sem=ag_send.at[side, hop, c],
            recv_sem=ag_recv.at[side, hop, c],
            device_id={"tp": peers[side]},
            device_id_type=MESH,
        )

    def own_copy(side, c):
        return pltpu.make_async_copy(
            slots.at[side, n - 1, c], dx.at[ag_rows(side, 0), columns(c)], own_sem.at[side, c]
        )

    barrier = pltpu.get_barrier_semaphore()
    for peer in peers:
        pl.semaphore_signal(barrier, inc=1, device_id={"tp": peer}, device_id_type=MESH)
    for copy in row_loads(0):
        copy.start()
    for i in range(PIECES):
        wd_load(i).start()
    for i in range(PIECES):
        for copy in wgu_loads(i):
            copy.start()
    pl.semaphore_wait(barrier, 2)

    def rs_step(step, _):
        for copy in row_loads(step):
            copy.wait()
        rows = pl.ds(pl.multiple_of(step * block, block), block)
        for i in range(PIECES):
            @pl.when(step == 0)
            def _():
                wd_load(i).wait()

            low, high = pl.ds(i * ff_piece, ff_piece), pl.ds(ff + i * ff_piece, ff_piece)
            d_hidden = dot_nt(dy_v[rows, :], w_d[low, :])
            hidden, back = jax.vjp(act, d_gu[rows, low].astype(F32), d_gu[rows, high].astype(F32))
            d_gate, d_up = back(d_hidden)
            hid[rows, low] = hidden.astype(BF16)
            d_gu[rows, low] = d_gate.astype(BF16)
            d_gu[rows, high] = d_up.astype(BF16)

        @pl.when(step < n - 1)
        def _():
            for copy in row_loads(step + 1):
                copy.start()

        for c in range(PIECES):
            @pl.when(step == 0)
            def _():
                for copy in wgu_loads(c):
                    copy.wait()

            part = dot_nt(d_gu[rows, :], w_gu[c * piece : (c + 1) * piece, :])

            @pl.when(step == 0)
            def _():
                for side in range(2):
                    slots[side, 0, c] = part[side * half : (side + 1) * half].astype(BF16)
                for side in range(2):
                    rs_copy(side, 0, c).start()

            @pl.when(step > 0)
            def _():
                term[c] = part

        @pl.when(step == n - 1)
        def _():
            for s in range(n):
                for side in range(2):
                    x_load(side, s).start()

        @pl.when(step > 0)
        def _():
            for c in range(PIECES):
                for side in range(2):
                    rs_copy(side, step - 1, c).wait_recv()
                    total = slots[side, step, c].astype(F32) + term[c, side * half : (side + 1) * half, :]
                    slots[side, step, c] = total.astype(BF16)

                @pl.when(step < n - 1)
                def _():
                    for side in range(2):
                        rs_copy(side, step, c).start()

                @pl.when(step == n - 1)
                def _():
                    for side in range(2):
                        ag_copy(side, 0, c, True).start()
                        own_copy(side, c).start()

        return 0

    lax.fori_loop(0, n, rs_step, 0)

    down_tiles = ff // TILE
    up_tiles = width // TILE
    down_units = down_tiles * (width // ff)
    units = down_units + 2 * up_tiles

    def out_copy(unit):
        slot = lax.rem(unit, 2)
        return pltpu.make_async_copy(stage.at[slot], dw_gate.at[pl.ds(0, TILE), :], out_sem.at[slot])

    def work(unit):
        slot = lax.rem(unit, 2)

        @pl.when(unit >= 2)
        def _():
            out_copy(unit).wait()

        @pl.when(unit < down_units)
        def _():
            row = pl.ds(pl.multiple_of(lax.rem(unit, down_tiles) * TILE, TILE), TILE)
            col = pl.ds(pl.multiple_of(lax.div(unit, down_tiles) * ff, ff), ff)
            stage[slot] = dot_tn(hid[:, row], dy_v[:, col]).astype(BF16)
            pltpu.make_async_copy(stage.at[slot], dw_down.at[row, col], out_sem.at[slot]).start()

        @pl.when(unit == down_units)
        def _():
            for s in range(n):
                for side in range(2):
                    x_load(side, s).wait()

        @pl.when(unit >= down_units)
        def _():
            which = lax.div(unit - down_units, up_tiles)
            row = pl.ds(pl.multiple_of(lax.rem(unit - down_units, up_tiles) * TILE, TILE), TILE)
            col = pl.ds(pl.multiple_of(which * ff, ff), ff)
            stage[slot] = dot_tn(w_gu[pl.ds(0, tokens), row], d_gu[:, col]).astype(BF16)
            for i, out in enumerate((dw_gate, dw_up)):
                @pl.when(which == i)
                def _():
                    pltpu.make_async_copy(stage.at[slot], out.at[row, :], out_sem.at[slot]).start()

    def ag_step(turn, _):
        @pl.when(turn < units)
        def _():
            work(turn)

        hop, c = lax.div(turn, PIECES), lax.rem(turn, PIECES)
        for side in range(2):
            ag_copy(side, hop, c, False).wait_recv()

            @pl.when(hop < n - 2)
            def _():
                ag_copy(side, hop + 1, c, False).start()

        return 0

    turns = (n - 1) * PIECES
    assert units <= turns and width == 2 * ff and tokens <= width
    lax.fori_loop(0, turns, ag_step, 0)

    for unit in (units - 2, units - 1):
        out_copy(unit).wait()

    def sends(hop, _):
        for side in range(2):
            for c in range(PIECES):
                rs_copy(side, hop, c).wait_send()
                ag_copy(side, hop, c, False).wait_send()
        return 0

    lax.fori_loop(0, n - 1, sends, 0)
    for side in range(2):
        for c in range(PIECES):
            own_copy(side, c).wait()


def solution(mesh):
    n = mesh.shape["tp"]

    def step(x, dy, gate, up, w_gate, w_up, w_down):
        tokens, width = x.shape
        ff = gate.shape[1]
        block, half, piece = tokens // n, tokens // n // 2, width // PIECES
        hbm = pl.BlockSpec(memory_space=pl.ANY)
        return pl.pallas_call(
            functools.partial(kernel, n),
            out_shape=[jax.ShapeDtypeStruct(a.shape, BF16) for a in (x, w_gate, w_up, w_down)],
            in_specs=[hbm] * 7,
            out_specs=[hbm] * 4,
            scratch_shapes=[
                pltpu.VMEM((width, 2 * ff), BF16),
                pltpu.VMEM((ff, width), BF16),
                pltpu.VMEM((tokens, 2 * ff), BF16),
                pltpu.VMEM((tokens, ff), BF16),
                pltpu.VMEM((tokens, width), BF16),
                pltpu.VMEM((PIECES, block, piece), F32),
                pltpu.VMEM((2, n, PIECES, half, piece), BF16),
                pltpu.VMEM((2, TILE, ff), BF16),
                pltpu.SemaphoreType.DMA((2, 6)),
                pltpu.SemaphoreType.DMA((PIECES,)),
                pltpu.SemaphoreType.DMA((PIECES, 2)),
                pltpu.SemaphoreType.DMA((n, 2)),
                pltpu.SemaphoreType.DMA((2,)),
                pltpu.SemaphoreType.DMA((2, PIECES)),
                pltpu.SemaphoreType.DMA((2, n, PIECES)),
                pltpu.SemaphoreType.DMA((2, n, PIECES)),
                pltpu.SemaphoreType.DMA((2, n, PIECES)),
                pltpu.SemaphoreType.DMA((2, n, PIECES)),
            ],
            compiler_params=pltpu.CompilerParams(
                collective_id=0, has_side_effects=True, vmem_limit_bytes=67_043_328
            ),
        )(x, dy, gate, up, w_gate, w_up, w_down)

    tokens, columns, rows = P("dp", None), P(None, "tp"), P("tp", None)
    return jax.shard_map(
        step,
        mesh=mesh,
        in_specs=(tokens, tokens, P("dp", "tp"), P("dp", "tp"), columns, columns, rows),
        out_specs=(tokens, P("dp", "tp"), P("dp", "tp"), P(("dp", "tp"), None)),
        check_vma=False,
    )
```

```python
import functools

import jax
import jax.numpy as jnp
from jax import lax
from jax.experimental import pallas as pl
from jax.experimental.pallas import tpu as pltpu
from jax.sharding import PartitionSpec as P

MESH = pl.DeviceIdType.MESH
F32 = jnp.float32
BF16 = jnp.bfloat16
PIECES = 3
TILE = 384


def act(gate, up):
    return jax.nn.gelu(gate) * up


def dot_nt(a, b):
    return lax.dot_general(a, b, (((1,), (1,)), ((), ())), preferred_element_type=F32)


def dot_tn(a, b):
    return lax.dot_general(a, b, (((0,), (0,)), ((), ())), preferred_element_type=F32)


def kernel(
    n,
    x, dy, gate, up, w_gate, w_up, w_down,
    dx, dw_gate, dw_up, dw_down, last_high, last_low,
    w_gu, w_d, d_gu, hid, dy_v, term, slots, stage,
    row_sem, wd_sem, wgu_sem, x_sem, out_sem, own_sem, rs_send, rs_recv, ag_send, ag_recv,
):
    tokens, width = dy_v.shape
    ff = w_d.shape[0]
    block = tokens // n
    half = block // 2
    piece = width // PIECES
    ff_piece = ff // PIECES
    me = lax.axis_index("tp")
    right, left = lax.rem(me + 1, n), lax.rem(me + n - 1, n)
    peers = (right, left)

    def rows_of(side, step):
        if side == 0:
            return pl.ds(pl.multiple_of(lax.rem(me - step + 2 * n, n) * block, block), half)
        return pl.ds(pl.multiple_of(lax.rem(me + step + n, n) * block + half, half), half)

    def held(side, step):
        return pl.ds(pl.multiple_of(step * block + side * half, half), half)

    def row_loads(step):
        parity = lax.rem(step, 2)
        copies = []
        for side in range(2):
            src, dst = rows_of(side, step), held(side, step)
            pairs = (
                (gate.at[src, :], d_gu.at[dst, pl.ds(0, ff)]),
                (up.at[src, :], d_gu.at[dst, pl.ds(ff, ff)]),
                (dy.at[src, :], dy_v.at[dst, :]),
            )
            for i, (a, b) in enumerate(pairs):
                copies.append((i, pltpu.make_async_copy(a, b, row_sem.at[parity, side * 3 + i])))
        return [copy for _, copy in sorted(copies, key=lambda pair: pair[0])]

    def wd_load(i):
        rows = pl.ds(i * ff_piece, ff_piece)
        return pltpu.make_async_copy(w_down.at[rows, :], w_d.at[rows, :], wd_sem.at[i])

    def wgu_loads(i):
        rows = pl.ds(i * piece, piece)
        return [
            pltpu.make_async_copy(w.at[rows, :], w_gu.at[rows, pl.ds(j * ff, ff)], wgu_sem.at[i, j])
            for j, w in enumerate((w_gate, w_up))
        ]

    def x_load(side, step):
        return pltpu.make_async_copy(x.at[rows_of(side, step), :], w_gu.at[held(side, step), :], x_sem.at[step, side])

    def rs_copy(side, step, c):
        return pltpu.make_async_remote_copy(
            src_ref=slots.at[side, step, c],
            dst_ref=slots.at[side, step + 1, c],
            send_sem=rs_send.at[side, step, c],
            recv_sem=rs_recv.at[side, step + 1, c],
            device_id={"tp": peers[side]},
            device_id_type=MESH,
        )

    def columns(c):
        return pl.ds(pl.multiple_of(c * piece, piece), piece)

    def ag_rows(side, hop):
        return rows_of(side, hop + n - 1)

    hops = n - 2

    def ag_copy(side, hop, c, first=False, last=False):
        place = dx.at[ag_rows(side, hop), columns(c)]
        return pltpu.make_async_remote_copy(
            src_ref=slots.at[side, n - 1, c] if first else place,
            dst_ref=(last_high, last_low)[side].at[:, columns(c)] if last else place,
            send_sem=ag_send.at[side, hop, c],
            recv_sem=ag_recv.at[side, hop, c],
            device_id={"tp": peers[side]},
            device_id_type=MESH,
        )

    def own_copy(side, c):
        return pltpu.make_async_copy(
            slots.at[side, n - 1, c], dx.at[ag_rows(side, 0), columns(c)], own_sem.at[side, c]
        )

    barrier = pltpu.get_barrier_semaphore()
    for peer in peers:
        pl.semaphore_signal(barrier, inc=1, device_id={"tp": peer}, device_id_type=MESH)
    for copy in row_loads(0):
        copy.start()
    for i in range(PIECES):
        wd_load(i).start()
    pl.semaphore_wait(barrier, 2)

    def rs_step(step, _):
        loads = row_loads(step)
        for copy in loads[:4]:
            copy.wait()
        rows = pl.ds(pl.multiple_of(step * block, block), block)
        for i in range(PIECES):
            low, high = pl.ds(i * ff_piece, ff_piece), pl.ds(ff + i * ff_piece, ff_piece)
            g = d_gu[rows, low].astype(F32)
            value, back = jax.vjp(jax.nn.gelu, g)
            (slope,) = back(jnp.ones_like(g))
            term[:, low] = slope
            term[:, high] = value
            hid[rows, low] = (value * d_gu[rows, high].astype(F32)).astype(BF16)
        for copy in loads[4:]:
            copy.wait()
        for i in range(PIECES):
            @pl.when(step == 0)
            def _():
                wd_load(i).wait()
                for copy in wgu_loads(i):
                    copy.start()

            low, high = pl.ds(i * ff_piece, ff_piece), pl.ds(ff + i * ff_piece, ff_piece)
            d_hidden = dot_nt(dy_v[rows, :], w_d[low, :])
            d_gu[rows, low] = (d_hidden * d_gu[rows, high].astype(F32) * term[:, low]).astype(BF16)
            d_gu[rows, high] = (d_hidden * term[:, high]).astype(BF16)

        for c in range(PIECES):
            @pl.when(step == 0)
            def _():
                for copy in wgu_loads(c):
                    copy.wait()

            part = dot_nt(d_gu[rows, :], w_gu[c * piece : (c + 1) * piece, :])

            @pl.when(step == 0)
            def _():
                for side in range(2):
                    slots[side, 0, c] = part[side * half : (side + 1) * half].astype(BF16)
                for side in range(2):
                    rs_copy(side, 0, c).start()

            @pl.when(step > 0)
            def _():
                term[:, c * piece : (c + 1) * piece] = part

        @pl.when(step < n - 1)
        def _():
            for copy in row_loads(step + 1):
                copy.start()

        @pl.when(step == n - 1)
        def _():
            for s in range(n):
                for side in range(2):
                    x_load(side, s).start()

        @pl.when(step > 0)
        def _():
            for c in range(PIECES):
                for side in range(2):
                    rs_copy(side, step - 1, c).wait_recv()
                    total = slots[side, step, c].astype(F32) + term[side * half : (side + 1) * half, c * piece : (c + 1) * piece]
                    slots[side, step, c] = total.astype(BF16)

                @pl.when(step < n - 1)
                def _():
                    for side in range(2):
                        rs_copy(side, step, c).start()

                @pl.when(step == n - 1)
                def _():
                    for side in range(2):
                        ag_copy(side, 0, c, first=True).start()
                        own_copy(side, c).start()

        return 0

    lax.fori_loop(0, n, rs_step, 0)

    down_tiles = ff // TILE
    up_tiles = width // TILE
    down_units = down_tiles * (width // ff)
    units = down_units + 2 * up_tiles

    def out_copy(unit):
        slot = lax.rem(unit, 2)
        return pltpu.make_async_copy(stage.at[slot], dw_gate.at[pl.ds(0, TILE), :], out_sem.at[slot])

    def work(unit):
        slot = lax.rem(unit, 2)

        @pl.when(unit >= 2)
        def _():
            out_copy(unit).wait()

        @pl.when(unit < down_units)
        def _():
            row = pl.ds(pl.multiple_of(lax.rem(unit, down_tiles) * TILE, TILE), TILE)
            col = pl.ds(pl.multiple_of(lax.div(unit, down_tiles) * ff, ff), ff)
            stage[slot] = dot_tn(hid[:, row], dy_v[:, col]).astype(BF16)
            pltpu.make_async_copy(stage.at[slot], dw_down.at[row, col], out_sem.at[slot]).start()

        @pl.when(unit == down_units)
        def _():
            for s in range(n):
                for side in range(2):
                    x_load(side, s).wait()

        @pl.when(unit >= down_units)
        def _():
            which = lax.div(unit - down_units, up_tiles)
            row = pl.ds(pl.multiple_of(lax.rem(unit - down_units, up_tiles) * TILE, TILE), TILE)
            col = pl.ds(pl.multiple_of(which * ff, ff), ff)
            stage[slot] = dot_tn(w_gu[pl.ds(0, tokens), row], d_gu[:, col]).astype(BF16)
            for i, out in enumerate((dw_gate, dw_up)):
                @pl.when(which == i)
                def _():
                    pltpu.make_async_copy(stage.at[slot], out.at[row, :], out_sem.at[slot]).start()

    def ag_step(turn, _):
        @pl.when(turn < units)
        def _():
            work(turn)

        hop, c = lax.div(turn, PIECES), lax.rem(turn, PIECES)
        for side in range(2):
            ag_copy(side, hop, c).wait_recv()

            @pl.when(hop < hops - 2)
            def _():
                ag_copy(side, hop + 1, c).start()

            @pl.when(hop == hops - 2)
            def _():
                ag_copy(side, hop + 1, c, last=True).start()

        return 0

    turns = hops * PIECES
    assert units <= turns and width == 2 * ff and tokens <= width
    lax.fori_loop(0, turns, ag_step, 0)

    for unit in (units - 2, units - 1):
        out_copy(unit).wait()

    def sends(hop, _):
        for side in range(2):
            for c in range(PIECES):
                rs_copy(side, hop, c).wait_send()

                @pl.when(hop < hops)
                def _():
                    ag_copy(side, hop, c).wait_send()

        return 0

    lax.fori_loop(0, n - 1, sends, 0)
    for side in range(2):
        for c in range(PIECES):
            own_copy(side, c).wait()


def outputs(
    n, dx_in, dw_gate_in, dw_up_in, dw_down_in, last_high, last_low, dx, dw_gate, dw_up, dw_down, wide, narrow, sems
):
    half = last_high.shape[0]
    block = 2 * half
    me = lax.axis_index("tp")
    jobs = []
    for i in range(n - 1):
        for side, last in enumerate((last_high, last_low)):
            place = lax.rem(me + 1 - i + n, n) if side == 0 else lax.rem(me - 1 + i + n, n)
            rows = pl.ds(pl.multiple_of(place * block + side * half, half), half)
            jobs.append((dx_in.at[rows, :] if i < n - 2 else last, wide, dx.at[rows, :]))
    for a, b, buffer in ((dw_down_in, dw_down, wide), (dw_gate_in, dw_gate, narrow), (dw_up_in, dw_up, narrow)):
        step = buffer.shape[1]
        for i in range(a.shape[0] // step):
            rows = pl.ds(i * step, step)
            jobs.append((a.at[rows, :], buffer, b.at[rows, :]))
    used = {id(wide): 0, id(narrow): 0}
    pairs = []
    for k, (src, buffer, dst) in enumerate(jobs):
        spot = buffer.at[used[id(buffer)]]
        used[id(buffer)] += 1
        pairs.append((pltpu.make_async_copy(src, spot, sems.at[0, k]), pltpu.make_async_copy(spot, dst, sems.at[1, k])))
    for load, _ in pairs:
        load.start()
    for load, store in pairs:
        load.wait()
        store.start()
    for _, store in pairs:
        store.wait()


def solution(mesh):
    n = mesh.shape["tp"]

    def step(x, dy, gate, up, w_gate, w_up, w_down):
        tokens, width = x.shape
        ff = gate.shape[1]
        block, half, piece = tokens // n, tokens // n // 2, width // PIECES
        hbm = pl.BlockSpec(memory_space=pl.ANY)
        results = [jax.ShapeDtypeStruct(a.shape, BF16) for a in (x, w_gate, w_up, w_down)]
        parts = pl.pallas_call(
            functools.partial(kernel, n),
            out_shape=results + [jax.ShapeDtypeStruct((half, width), BF16)] * 2,
            in_specs=[hbm] * 7,
            out_specs=[hbm] * 6,
            scratch_shapes=[
                pltpu.VMEM((width, 2 * ff), BF16),
                pltpu.VMEM((ff, width), BF16),
                pltpu.VMEM((tokens, 2 * ff), BF16),
                pltpu.VMEM((tokens, ff), BF16),
                pltpu.VMEM((tokens, width), BF16),
                pltpu.VMEM((block, width), F32),
                pltpu.VMEM((2, n, PIECES, half, piece), BF16),
                pltpu.VMEM((2, TILE, ff), BF16),
                pltpu.SemaphoreType.DMA((2, 6)),
                pltpu.SemaphoreType.DMA((PIECES,)),
                pltpu.SemaphoreType.DMA((PIECES, 2)),
                pltpu.SemaphoreType.DMA((n, 2)),
                pltpu.SemaphoreType.DMA((2,)),
                pltpu.SemaphoreType.DMA((2, PIECES)),
                pltpu.SemaphoreType.DMA((2, n, PIECES)),
                pltpu.SemaphoreType.DMA((2, n, PIECES)),
                pltpu.SemaphoreType.DMA((2, n, PIECES)),
                pltpu.SemaphoreType.DMA((2, n, PIECES)),
            ],
            compiler_params=pltpu.CompilerParams(
                collective_id=0, has_side_effects=True, vmem_limit_bytes=67_043_328
            ),
        )(x, dy, gate, up, w_gate, w_up, w_down)
        last_high, last_low = parts[4:]
        high = lax.ppermute(last_high, "tp", [(i, (i + 1) % n) for i in range(n)])
        low = lax.ppermute(last_low, "tp", [(i, (i - 1) % n) for i in range(n)])
        wide = 2 * (n - 1) + ff // half
        narrow = 2 * (width // block)
        dx, dw_gate, dw_up, dw_down = pl.pallas_call(
            functools.partial(outputs, n),
            out_shape=results,
            in_specs=[hbm] * 6,
            out_specs=[hbm] * 4,
            scratch_shapes=[
                pltpu.VMEM((wide, half, width), BF16),
                pltpu.VMEM((narrow, block, ff), BF16),
                pltpu.SemaphoreType.DMA((2, wide + narrow)),
            ],
            cost_estimate=pl.CostEstimate(flops=2**34, bytes_accessed=2**25, transcendentals=0),
            compiler_params=pltpu.CompilerParams(has_side_effects=True),
        )(*parts)
        me = lax.axis_index("tp")
        dx = lax.dynamic_update_slice(dx, high, (lax.rem(me + 2, n) * block, 0))
        dx = lax.dynamic_update_slice(dx, low, (lax.rem(me - 2 + n, n) * block + half, 0))
        return dx, dw_gate, dw_up, dw_down

    tokens, columns, rows = P("dp", None), P(None, "tp"), P("tp", None)
    return jax.shard_map(
        step,
        mesh=mesh,
        in_specs=(tokens, tokens, P("dp", "tp"), P("dp", "tp"), columns, columns, rows),
        out_specs=(tokens, P("dp", "tp"), P("dp", "tp"), P(("dp", "tp"), None)),
        check_vma=False,
    )
```

```python
import functools

import jax
import jax.numpy as jnp
from jax import lax
from jax.experimental import pallas as pl
from jax.experimental.pallas import tpu as pltpu
from jax.sharding import PartitionSpec as P

MESH = pl.DeviceIdType.MESH
F32 = jnp.float32
BF16 = jnp.bfloat16
PIECES = 3
FIRST = 3
TILE = 384


def dot_nt(a, b):
    return lax.dot_general(a, b, (((1,), (1,)), ((), ())), preferred_element_type=F32)


def dot_tn(a, b):
    return lax.dot_general(a, b, (((0,), (0,)), ((), ())), preferred_element_type=F32)


def kernel(
    n,
    x, dy, gate, up, w_gate, w_up, w_down,
    dx, dw_gate, dw_up, dw_down, last,
    w_gu, w_d, d_gu, hid, dy_v, term, slots, stage,
    row_sem, wd_sem, wgu_sem, x_sem, out_sem, own_sem, rs_send, rs_recv, ag_send, ag_recv,
):
    tokens, width = dy_v.shape
    ff = w_d.shape[0]
    block = tokens // n
    piece = width // PIECES
    first = piece // FIRST
    ff_piece = ff // PIECES
    me = lax.axis_index("tp")
    ahead = 1 - 2 * lax.rem(lax.axis_index("dp"), 2)
    peer = lax.rem(me + ahead + n, n)
    behind = lax.rem(me - ahead + n, n)
    hops = n - 2

    def block_rows(step):
        return pl.ds(pl.multiple_of(lax.rem(me - ahead * step + 2 * n, n) * block, block), block)

    def held(step):
        return pl.ds(pl.multiple_of(step * block, block), block)

    def row_loads(step):
        parity = lax.rem(step, 2)
        src, dst = block_rows(step), held(step)
        pairs = (
            (gate.at[src, :], d_gu.at[dst, pl.ds(0, ff)]),
            (up.at[src, :], d_gu.at[dst, pl.ds(ff, ff)]),
            (dy.at[src, :], dy_v.at[dst, :]),
        )
        return [pltpu.make_async_copy(a, b, row_sem.at[parity, i]) for i, (a, b) in enumerate(pairs)]

    def wd_load(i):
        rows = pl.ds(i * ff_piece, ff_piece)
        return pltpu.make_async_copy(w_down.at[rows, :], w_d.at[rows, :], wd_sem.at[i])

    tiles = [(i * first, first) for i in range(FIRST)] + [(c * piece, piece) for c in range(1, PIECES)]

    def wgu_loads(i):
        rows = pl.ds(*tiles[i])
        return [
            pltpu.make_async_copy(w.at[rows, :], w_gu.at[rows, pl.ds(j * ff, ff)], wgu_sem.at[i, j])
            for j, w in enumerate((w_gate, w_up))
        ]

    def x_load(step):
        return pltpu.make_async_copy(x.at[block_rows(step), :], w_gu.at[held(step), :], x_sem.at[step])

    def rs_copy(step, c, part=None):
        part = slice(None) if part is None else part
        return pltpu.make_async_remote_copy(
            src_ref=slots.at[step, c, :, part],
            dst_ref=slots.at[step + 1, c, :, part],
            send_sem=rs_send.at[step, c],
            recv_sem=rs_recv.at[step + 1, c],
            device_id={"tp": peer},
            device_id_type=MESH,
        )

    def columns(c):
        return pl.ds(pl.multiple_of(c * piece, piece), piece)

    def ag_copy(hop, c, own=False, final=False):
        place = dx.at[block_rows(hop + n - 1), columns(c)]
        return pltpu.make_async_remote_copy(
            src_ref=slots.at[n - 1, c] if own else place,
            dst_ref=last.at[:, columns(c)] if final else place,
            send_sem=ag_send.at[hop, c],
            recv_sem=ag_recv.at[hop, c],
            device_id={"tp": peer},
            device_id_type=MESH,
        )

    def own_copy(c):
        return pltpu.make_async_copy(slots.at[n - 1, c], dx.at[block_rows(n - 1), columns(c)], own_sem.at[c])

    barrier = pltpu.get_barrier_semaphore()
    for other in (peer, behind):
        pl.semaphore_signal(barrier, inc=1, device_id={"tp": other}, device_id_type=MESH)
    for copy in row_loads(0):
        copy.start()
    for i in range(PIECES):
        wd_load(i).start()
    pl.semaphore_wait(barrier, 2)

    def rs_step(step, _):
        loads = row_loads(step)
        for copy in loads[:2]:
            copy.wait()
        rows = held(step)
        for i in range(PIECES):
            low, high = pl.ds(i * ff_piece, ff_piece), pl.ds(ff + i * ff_piece, ff_piece)
            g = d_gu[rows, low].astype(F32)
            value, back = jax.vjp(jax.nn.gelu, g)
            (slope,) = back(jnp.ones_like(g))
            term[:, low] = slope
            term[:, high] = value
            hid[rows, low] = (value * d_gu[rows, high].astype(F32)).astype(BF16)
        loads[2].wait()
        for i in range(PIECES):
            @pl.when(step == 0)
            def _():
                wd_load(i).wait()
                for tile in ((0, 1), (2,), (3,))[i]:
                    for copy in wgu_loads(tile):
                        copy.start()

            low, high = pl.ds(i * ff_piece, ff_piece), pl.ds(ff + i * ff_piece, ff_piece)
            d_hidden = dot_nt(dy_v[rows, :], w_d[low, :])
            d_gu[rows, low] = (d_hidden * d_gu[rows, high].astype(F32) * term[:, low]).astype(BF16)
            d_gu[rows, high] = (d_hidden * term[:, high]).astype(BF16)

        for i, (start, size) in enumerate(tiles):
            @pl.when(step == 0)
            def _():
                for copy in wgu_loads(i):
                    copy.wait()
                if i == 0:
                    for copy in wgu_loads(4):
                        copy.start()

            part = dot_nt(d_gu[rows, :], w_gu[start : start + size, :])

            @pl.when(step == 0)
            def _():
                c = start // piece
                cols = slice(start - c * piece, start - c * piece + size)
                slots[0, c, :, cols] = part.astype(BF16)
                rs_copy(0, c, cols).start()

            @pl.when(step > 0)
            def _():
                term[:, start : start + size] = part

        @pl.when(step < n - 1)
        def _():
            for copy in row_loads(step + 1):
                copy.start()

        @pl.when(step == n - 1)
        def _():
            for s in range(n):
                x_load(s).start()

        @pl.when(step > 0)
        def _():
            for c in range(PIECES):
                rs_copy(step - 1, c).wait_recv()
                total = slots[step, c].astype(F32) + term[:, c * piece : (c + 1) * piece]
                slots[step, c] = total.astype(BF16)

                @pl.when(step < n - 1)
                def _():
                    rs_copy(step, c).start()

                @pl.when(step == n - 1)
                def _():
                    ag_copy(0, c, own=True).start()
                    own_copy(c).start()

        return 0

    lax.fori_loop(0, n, rs_step, 0)

    down_tiles = ff // TILE
    up_tiles = width // TILE
    down_units = down_tiles * (width // ff)
    units = down_units + 2 * up_tiles

    def out_copy(unit):
        slot = lax.rem(unit, 2)
        return pltpu.make_async_copy(stage.at[slot], dw_gate.at[pl.ds(0, TILE), :], out_sem.at[slot])

    def work(unit):
        slot = lax.rem(unit, 2)

        @pl.when(unit >= 2)
        def _():
            out_copy(unit).wait()

        @pl.when(unit < down_units)
        def _():
            row = pl.ds(pl.multiple_of(lax.rem(unit, down_tiles) * TILE, TILE), TILE)
            col = pl.ds(pl.multiple_of(lax.div(unit, down_tiles) * ff, ff), ff)
            stage[slot] = dot_tn(hid[:, row], dy_v[:, col]).astype(BF16)
            pltpu.make_async_copy(stage.at[slot], dw_down.at[row, col], out_sem.at[slot]).start()

        @pl.when(unit == down_units)
        def _():
            for s in range(n):
                x_load(s).wait()

        @pl.when(unit >= down_units)
        def _():
            which = lax.div(unit - down_units, up_tiles)
            row = pl.ds(pl.multiple_of(lax.rem(unit - down_units, up_tiles) * TILE, TILE), TILE)
            col = pl.ds(pl.multiple_of(which * ff, ff), ff)
            stage[slot] = dot_tn(w_gu[pl.ds(0, tokens), row], d_gu[:, col]).astype(BF16)
            for i, out in enumerate((dw_gate, dw_up)):
                @pl.when(which == i)
                def _():
                    pltpu.make_async_copy(stage.at[slot], out.at[row, :], out_sem.at[slot]).start()

    def ag_step(turn, _):
        @pl.when(turn < units)
        def _():
            work(turn)

        hop, c = lax.div(turn, PIECES), lax.rem(turn, PIECES)
        ag_copy(hop, c).wait_recv()

        @pl.when(hop < hops - 2)
        def _():
            ag_copy(hop + 1, c).start()

        @pl.when(hop == hops - 2)
        def _():
            ag_copy(hop + 1, c, final=True).start()

        return 0

    turns = hops * PIECES
    assert units <= turns and width == 2 * ff and tokens <= width
    lax.fori_loop(0, turns, ag_step, 0)

    for unit in (units - 2, units - 1):
        out_copy(unit).wait()

    def sends(hop, _):
        for c in range(PIECES):
            rs_copy(hop, c).wait_send()

            @pl.when(hop < hops)
            def _():
                ag_copy(hop, c).wait_send()

        return 0

    lax.fori_loop(0, n - 1, sends, 0)
    for c in range(PIECES):
        own_copy(c).wait()


def outputs(n, dx_in, dw_gate_in, dw_up_in, dw_down_in, last, dx, dw_gate, dw_up, dw_down, wide, narrow, sems):
    block = last.shape[0]
    me = lax.axis_index("tp")
    ahead = 1 - 2 * lax.rem(lax.axis_index("dp"), 2)
    jobs = []
    for i in range(n - 1):
        rows = pl.ds(pl.multiple_of(lax.rem(me + ahead - ahead * i + n, n) * block, block), block)
        jobs.append((dx_in.at[rows, :] if i < n - 2 else last, wide.at[pl.ds(i * block, block), :], dx.at[rows, :]))
    spot = (n - 1) * block
    for i in range(dw_down.shape[0] // TILE):
        rows = pl.ds(i * TILE, TILE)
        jobs.append((dw_down_in.at[rows, :], wide.at[pl.ds(spot + i * TILE, TILE), :], dw_down.at[rows, :]))
    step = 2 * TILE
    for j, (a, b) in enumerate(((dw_gate_in, dw_gate), (dw_up_in, dw_up))):
        for i in range(b.shape[0] // step):
            rows = pl.ds(i * step, step)
            jobs.append((a.at[rows, :], narrow.at[j, rows, :], b.at[rows, :]))
    loads = [pltpu.make_async_copy(a, v, sems.at[0, k]) for k, (a, v, _) in enumerate(jobs)]
    stores = [pltpu.make_async_copy(v, b, sems.at[1, k]) for k, (_, v, b) in enumerate(jobs)]
    for load in loads:
        load.start()
    for load, store in zip(loads, stores):
        load.wait()
        store.start()
    for store in stores:
        store.wait()


def solution(mesh):
    n, groups = mesh.shape["tp"], mesh.shape["dp"]

    def step(x, dy, gate, up, w_gate, w_up, w_down):
        tokens, width = x.shape
        ff = gate.shape[1]
        block, piece = tokens // n, width // PIECES
        hbm = pl.BlockSpec(memory_space=pl.ANY)
        results = [jax.ShapeDtypeStruct(a.shape, BF16) for a in (x, w_gate, w_up, w_down)]
        parts = pl.pallas_call(
            functools.partial(kernel, n),
            out_shape=results + [jax.ShapeDtypeStruct((block, width), BF16)],
            in_specs=[hbm] * 7,
            out_specs=[hbm] * 5,
            scratch_shapes=[
                pltpu.VMEM((width, 2 * ff), BF16),
                pltpu.VMEM((ff, width), BF16),
                pltpu.VMEM((tokens, 2 * ff), BF16),
                pltpu.VMEM((tokens, ff), BF16),
                pltpu.VMEM((tokens, width), BF16),
                pltpu.VMEM((block, width), F32),
                pltpu.VMEM((n, PIECES, block, piece), BF16),
                pltpu.VMEM((2, TILE, ff), BF16),
                pltpu.SemaphoreType.DMA((2, 3)),
                pltpu.SemaphoreType.DMA((PIECES,)),
                pltpu.SemaphoreType.DMA((FIRST + PIECES - 1, 2)),
                pltpu.SemaphoreType.DMA((n,)),
                pltpu.SemaphoreType.DMA((2,)),
                pltpu.SemaphoreType.DMA((PIECES,)),
                pltpu.SemaphoreType.DMA((n, PIECES)),
                pltpu.SemaphoreType.DMA((n, PIECES)),
                pltpu.SemaphoreType.DMA((n, PIECES)),
                pltpu.SemaphoreType.DMA((n, PIECES)),
            ],
            compiler_params=pltpu.CompilerParams(
                collective_id=0, has_side_effects=True, vmem_limit_bytes=67_043_328
            ),
        )(x, dy, gate, up, w_gate, w_up, w_down)
        ring = [(d * n + i, d * n + (i + 1 - 2 * (d % 2)) % n) for d in range(groups) for i in range(n)]
        final = lax.ppermute(parts[4], ("dp", "tp"), ring)
        dx, dw_gate, dw_up, dw_down = pl.pallas_call(
            functools.partial(outputs, n),
            out_shape=results,
            in_specs=[hbm] * 5,
            out_specs=[hbm] * 4,
            scratch_shapes=[
                pltpu.VMEM(((n - 1) * block + ff, width), BF16),
                pltpu.VMEM((2, width, ff), BF16),
                pltpu.SemaphoreType.DMA((2, n - 1 + ff // TILE + width // TILE)),
            ],
            cost_estimate=pl.CostEstimate(flops=2**34, bytes_accessed=2**25, transcendentals=0),
            compiler_params=pltpu.CompilerParams(has_side_effects=True),
        )(*parts)
        me = lax.axis_index("tp")
        ahead = 1 - 2 * lax.rem(lax.axis_index("dp"), 2)
        dx = lax.dynamic_update_slice(dx, final, (lax.rem(me + 2 * ahead + n, n) * block, 0))
        return dx, dw_gate, dw_up, dw_down

    tokens, columns, rows = P("dp", None), P(None, "tp"), P("tp", None)
    return jax.shard_map(
        step,
        mesh=mesh,
        in_specs=(tokens, tokens, P("dp", "tp"), P("dp", "tp"), columns, columns, rows),
        out_specs=(tokens, P("dp", "tp"), P("dp", "tp"), P(("dp", "tp"), None)),
        check_vma=False,
    )
```

```python
import functools

import jax
import jax.numpy as jnp
from jax import lax
from jax.experimental import pallas as pl
from jax.experimental.pallas import tpu as pltpu
from jax.sharding import PartitionSpec as P

MESH = pl.DeviceIdType.MESH
F32 = jnp.float32
BF16 = jnp.bfloat16
PIECES = 2
FIRST = 256
FF_PIECES = 3
TILE = 384


def dot_nt(a, b):
    return lax.dot_general(a, b, (((1,), (1,)), ((), ())), preferred_element_type=F32)


def dot_tn(a, b):
    return lax.dot_general(a, b, (((0,), (0,)), ((), ())), preferred_element_type=F32)


def kernel(
    n,
    x, dy, gate, up, w_gate, w_up, w_down,
    dx, dw_gate, dw_up, dw_down, last,
    w_gu, w_d, d_gu, hid, dy_v, term, slots, stage,
    row_sem, wd_sem, wgu_sem, x_sem, out_sem, own_sem, rs_send, rs_recv, ag_send, ag_recv,
):
    tokens, width = dy_v.shape
    ff = w_d.shape[0]
    block = tokens // n
    piece = width // PIECES
    ff_piece = ff // FF_PIECES
    me = lax.axis_index("tp")
    ahead = 1 - 2 * lax.rem(lax.axis_index("dp"), 2)
    peer = lax.rem(me + ahead + n, n)
    behind = lax.rem(me - ahead + n, n)
    hops = n - 2

    def block_rows(step):
        return pl.ds(pl.multiple_of(lax.rem(me - ahead * step + 2 * n, n) * block, block), block)

    def held(step):
        return pl.ds(pl.multiple_of(step * block, block), block)

    def row_loads(step):
        parity = lax.rem(step, 2)
        src, dst = block_rows(step), held(step)
        pairs = (
            (gate.at[src, :], d_gu.at[dst, pl.ds(0, ff)]),
            (up.at[src, :], d_gu.at[dst, pl.ds(ff, ff)]),
            (dy.at[src, :], dy_v.at[dst, :]),
        )
        return [pltpu.make_async_copy(a, b, row_sem.at[parity, i]) for i, (a, b) in enumerate(pairs)]

    def wd_load(i):
        rows = pl.ds(i * ff_piece, ff_piece)
        return pltpu.make_async_copy(w_down.at[rows, :], w_d.at[rows, :], wd_sem.at[i])

    tiles = [(0, FIRST), (FIRST, piece - FIRST)] + [(c * piece, piece) for c in range(1, PIECES)]

    def wgu_loads(i):
        rows = pl.ds(*tiles[i])
        return [
            pltpu.make_async_copy(w.at[rows, :], w_gu.at[rows, pl.ds(j * ff, ff)], wgu_sem.at[i, j])
            for j, w in enumerate((w_gate, w_up))
        ]

    def x_load(step):
        return pltpu.make_async_copy(x.at[block_rows(step), :], w_gu.at[held(step), :], x_sem.at[step])

    def rs_copy(step, c, part=None):
        part = slice(None) if part is None else part
        return pltpu.make_async_remote_copy(
            src_ref=slots.at[step, c, :, part],
            dst_ref=slots.at[step + 1, c, :, part],
            send_sem=rs_send.at[step, c],
            recv_sem=rs_recv.at[step + 1, c],
            device_id={"tp": peer},
            device_id_type=MESH,
        )

    def columns(c):
        return pl.ds(pl.multiple_of(c * piece, piece), piece)

    def ag_copy(hop, c, own=False, final=False):
        place = dx.at[block_rows(hop + n - 1), columns(c)]
        return pltpu.make_async_remote_copy(
            src_ref=slots.at[n - 1, c] if own else place,
            dst_ref=last.at[:, columns(c)] if final else place,
            send_sem=ag_send.at[hop, c],
            recv_sem=ag_recv.at[hop, c],
            device_id={"tp": peer},
            device_id_type=MESH,
        )

    def own_copy(c):
        return pltpu.make_async_copy(slots.at[n - 1, c], dx.at[block_rows(n - 1), columns(c)], own_sem.at[c])

    barrier = pltpu.get_barrier_semaphore()
    for other in (peer, behind):
        pl.semaphore_signal(barrier, inc=1, device_id={"tp": other}, device_id_type=MESH)
    for copy in row_loads(0):
        copy.start()
    for i in range(FF_PIECES):
        wd_load(i).start()
    pl.semaphore_wait(barrier, 2)

    def rs_step(step, _):
        loads = row_loads(step)
        for copy in loads[:2]:
            copy.wait()
        rows = held(step)
        for i in range(FF_PIECES):
            low, high = pl.ds(i * ff_piece, ff_piece), pl.ds(ff + i * ff_piece, ff_piece)
            g = d_gu[rows, low].astype(F32)
            value, back = jax.vjp(jax.nn.gelu, g)
            (slope,) = back(jnp.ones_like(g))
            term[:, low] = slope
            term[:, high] = value
            hid[rows, low] = (value * d_gu[rows, high].astype(F32)).astype(BF16)
        loads[2].wait()
        for i in range(FF_PIECES):
            @pl.when(step == 0)
            def _():
                wd_load(i).wait()
                for copy in wgu_loads(i):
                    copy.start()

            low, high = pl.ds(i * ff_piece, ff_piece), pl.ds(ff + i * ff_piece, ff_piece)
            d_hidden = dot_nt(dy_v[rows, :], w_d[low, :])
            d_gu[rows, low] = (d_hidden * d_gu[rows, high].astype(F32) * term[:, low]).astype(BF16)
            d_gu[rows, high] = (d_hidden * term[:, high]).astype(BF16)

        for i, (start, size) in enumerate(tiles):
            @pl.when(step == 0)
            def _():
                for copy in wgu_loads(i):
                    copy.wait()

            part = dot_nt(d_gu[rows, :], w_gu[start : start + size, :])

            @pl.when(step == 0)
            def _():
                c = start // piece
                cols = slice(start - c * piece, start - c * piece + size)
                slots[0, c, :, cols] = part.astype(BF16)
                rs_copy(0, c, cols).start()

            @pl.when(step > 0)
            def _():
                term[:, start : start + size] = part

        @pl.when(step < n - 1)
        def _():
            for copy in row_loads(step + 1):
                copy.start()

        @pl.when(step == n - 1)
        def _():
            for s in range(n):
                x_load(s).start()

        @pl.when(step > 0)
        def _():
            for c in range(PIECES):
                rs_copy(step - 1, c).wait_recv()
                total = slots[step, c].astype(F32) + term[:, c * piece : (c + 1) * piece]
                slots[step, c] = total.astype(BF16)

                @pl.when(step < n - 1)
                def _():
                    rs_copy(step, c).start()

                @pl.when(step == n - 1)
                def _():
                    ag_copy(0, c, own=True).start()
                    own_copy(c).start()

        return 0

    lax.fori_loop(0, n, rs_step, 0)

    down_tiles = ff // TILE
    up_tiles = width // TILE
    down_units = down_tiles * (width // ff)
    units = down_units + 2 * up_tiles

    def out_copy(unit):
        slot = lax.rem(unit, 2)
        return pltpu.make_async_copy(stage.at[slot], dw_gate.at[pl.ds(0, TILE), :], out_sem.at[slot])

    def work(unit):
        slot = lax.rem(unit, 2)

        @pl.when(unit >= 2)
        def _():
            out_copy(unit).wait()

        @pl.when(unit < down_units)
        def _():
            row = pl.ds(pl.multiple_of(lax.rem(unit, down_tiles) * TILE, TILE), TILE)
            col = pl.ds(pl.multiple_of(lax.div(unit, down_tiles) * ff, ff), ff)
            stage[slot] = dot_tn(hid[:, row], dy_v[:, col]).astype(BF16)
            pltpu.make_async_copy(stage.at[slot], dw_down.at[row, col], out_sem.at[slot]).start()

        @pl.when(unit == down_units)
        def _():
            for s in range(n):
                x_load(s).wait()

        @pl.when(unit >= down_units)
        def _():
            which = lax.div(unit - down_units, up_tiles)
            row = pl.ds(pl.multiple_of(lax.rem(unit - down_units, up_tiles) * TILE, TILE), TILE)
            col = pl.ds(pl.multiple_of(which * ff, ff), ff)
            stage[slot] = dot_tn(w_gu[pl.ds(0, tokens), row], d_gu[:, col]).astype(BF16)
            for i, out in enumerate((dw_gate, dw_up)):
                @pl.when(which == i)
                def _():
                    pltpu.make_async_copy(stage.at[slot], out.at[row, :], out_sem.at[slot]).start()

    turns = hops * PIECES
    per_turn = -(-units // turns)

    def ag_step(turn, _):
        for k in range(per_turn):
            @pl.when(turn * per_turn + k < units)
            def _():
                work(turn * per_turn + k)

        hop, c = lax.div(turn, PIECES), lax.rem(turn, PIECES)
        ag_copy(hop, c).wait_recv()

        @pl.when(hop < hops - 2)
        def _():
            ag_copy(hop + 1, c).start()

        @pl.when(hop == hops - 2)
        def _():
            ag_copy(hop + 1, c, final=True).start()

        return 0

    assert FF_PIECES == PIECES + 1 and width == 2 * ff and tokens <= width
    lax.fori_loop(0, turns, ag_step, 0)

    for unit in (units - 2, units - 1):
        out_copy(unit).wait()

    def sends(hop, _):
        for c in range(PIECES):
            rs_copy(hop, c).wait_send()

            @pl.when(hop < hops)
            def _():
                ag_copy(hop, c).wait_send()

        return 0

    lax.fori_loop(0, n - 1, sends, 0)
    for c in range(PIECES):
        own_copy(c).wait()


def outputs(n, dx_in, dw_gate_in, dw_up_in, dw_down_in, last, dx, dw_gate, dw_up, dw_down, wide, narrow, sems):
    block = last.shape[0]
    me = lax.axis_index("tp")
    ahead = 1 - 2 * lax.rem(lax.axis_index("dp"), 2)
    jobs = []
    for i in range(n - 1):
        rows = pl.ds(pl.multiple_of(lax.rem(me + ahead - ahead * i + n, n) * block, block), block)
        jobs.append((dx_in.at[rows, :] if i < n - 2 else last, wide.at[pl.ds(i * block, block), :], dx.at[rows, :]))
    spot = (n - 1) * block
    for i in range(dw_down.shape[0] // TILE):
        rows = pl.ds(i * TILE, TILE)
        jobs.append((dw_down_in.at[rows, :], wide.at[pl.ds(spot + i * TILE, TILE), :], dw_down.at[rows, :]))
    step = 2 * TILE
    for j, (a, b) in enumerate(((dw_gate_in, dw_gate), (dw_up_in, dw_up))):
        for i in range(b.shape[0] // step):
            rows = pl.ds(i * step, step)
            jobs.append((a.at[rows, :], narrow.at[j, rows, :], b.at[rows, :]))
    loads = [pltpu.make_async_copy(a, v, sems.at[0, k]) for k, (a, v, _) in enumerate(jobs)]
    stores = [pltpu.make_async_copy(v, b, sems.at[1, k]) for k, (_, v, b) in enumerate(jobs)]
    for load in loads:
        load.start()
    for load, store in zip(loads, stores):
        load.wait()
        store.start()
    for store in stores:
        store.wait()


def solution(mesh):
    n, groups = mesh.shape["tp"], mesh.shape["dp"]

    def step(x, dy, gate, up, w_gate, w_up, w_down):
        tokens, width = x.shape
        ff = gate.shape[1]
        block, piece = tokens // n, width // PIECES
        hbm = pl.BlockSpec(memory_space=pl.ANY)
        results = [jax.ShapeDtypeStruct(a.shape, BF16) for a in (x, w_gate, w_up, w_down)]
        parts = pl.pallas_call(
            functools.partial(kernel, n),
            out_shape=results + [jax.ShapeDtypeStruct((block, width), BF16)],
            in_specs=[hbm] * 7,
            out_specs=[hbm] * 5,
            scratch_shapes=[
                pltpu.VMEM((width, 2 * ff), BF16),
                pltpu.VMEM((ff, width), BF16),
                pltpu.VMEM((tokens, 2 * ff), BF16),
                pltpu.VMEM((tokens, ff), BF16),
                pltpu.VMEM((tokens, width), BF16),
                pltpu.VMEM((block, width), F32),
                pltpu.VMEM((n, PIECES, block, piece), BF16),
                pltpu.VMEM((2, TILE, ff), BF16),
                pltpu.SemaphoreType.DMA((2, 3)),
                pltpu.SemaphoreType.DMA((FF_PIECES,)),
                pltpu.SemaphoreType.DMA((PIECES + 1, 2)),
                pltpu.SemaphoreType.DMA((n,)),
                pltpu.SemaphoreType.DMA((2,)),
                pltpu.SemaphoreType.DMA((PIECES,)),
                pltpu.SemaphoreType.DMA((n, PIECES)),
                pltpu.SemaphoreType.DMA((n, PIECES)),
                pltpu.SemaphoreType.DMA((n, PIECES)),
                pltpu.SemaphoreType.DMA((n, PIECES)),
            ],
            compiler_params=pltpu.CompilerParams(
                collective_id=0, has_side_effects=True, vmem_limit_bytes=67_043_328
            ),
        )(x, dy, gate, up, w_gate, w_up, w_down)
        ring = [(d * n + i, d * n + (i + 1 - 2 * (d % 2)) % n) for d in range(groups) for i in range(n)]
        final = lax.ppermute(parts[4], ("dp", "tp"), ring)
        dx, dw_gate, dw_up, dw_down = pl.pallas_call(
            functools.partial(outputs, n),
            out_shape=results,
            in_specs=[hbm] * 5,
            out_specs=[hbm] * 4,
            scratch_shapes=[
                pltpu.VMEM(((n - 1) * block + ff, width), BF16),
                pltpu.VMEM((2, width, ff), BF16),
                pltpu.SemaphoreType.DMA((2, n - 1 + ff // TILE + width // TILE)),
            ],
            cost_estimate=pl.CostEstimate(flops=2**34, bytes_accessed=2**25, transcendentals=0),
            compiler_params=pltpu.CompilerParams(has_side_effects=True),
        )(*parts)
        me = lax.axis_index("tp")
        ahead = 1 - 2 * lax.rem(lax.axis_index("dp"), 2)
        dx = lax.dynamic_update_slice(dx, final, (lax.rem(me + 2 * ahead + n, n) * block, 0))
        return dx, dw_gate, dw_up, dw_down

    tokens, columns, rows = P("dp", None), P(None, "tp"), P("tp", None)
    return jax.shard_map(
        step,
        mesh=mesh,
        in_specs=(tokens, tokens, P("dp", "tp"), P("dp", "tp"), columns, columns, rows),
        out_specs=(tokens, P("dp", "tp"), P("dp", "tp"), P(("dp", "tp"), None)),
        check_vma=False,
    )
```

```python
import functools

import jax
import jax.numpy as jnp
from jax import lax
from jax.experimental import pallas as pl
from jax.experimental.pallas import tpu as pltpu
from jax.sharding import PartitionSpec as P

MESH = pl.DeviceIdType.MESH
F32 = jnp.float32
BF16 = jnp.bfloat16
PIECES = 2
FIRST = 256
FF_PIECES = 3
TILE = 384


def dot_nt(a, b):
    return lax.dot_general(a, b, (((1,), (1,)), ((), ())), preferred_element_type=F32)


def dot_tn(a, b):
    return lax.dot_general(a, b, (((0,), (0,)), ((), ())), preferred_element_type=F32)


def kernel(
    n,
    x, dy, gate, up, w_gate, w_up, w_down,
    dx, dw_gate, dw_up, dw_down, early, late,
    w_gu, w_d, d_gu, hid, dy_v, term, slots, stage,
    row_sem, wd_sem, wgu_sem, x_sem, out_sem, own_sem, rs_send, rs_recv, ag_send, ag_recv,
):
    tokens, width = dy_v.shape
    ff = w_d.shape[0]
    block = tokens // n
    piece = width // PIECES
    ff_piece = ff // FF_PIECES
    me = lax.axis_index("tp")
    ahead = 1 - 2 * lax.rem(lax.axis_index("dp"), 2)
    peer = lax.rem(me + ahead + n, n)
    behind = lax.rem(me - ahead + n, n)
    hops = n - 2
    turns = (hops - 1) * PIECES + 1

    def block_rows(step):
        return pl.ds(pl.multiple_of(lax.rem(me - ahead * step + 2 * n, n) * block, block), block)

    def held(step):
        return pl.ds(pl.multiple_of(step * block, block), block)

    def row_loads(step):
        parity = lax.rem(step, 2)
        src, dst = block_rows(step), held(step)
        pairs = (
            (gate.at[src, :], d_gu.at[dst, pl.ds(0, ff)]),
            (up.at[src, :], d_gu.at[dst, pl.ds(ff, ff)]),
            (dy.at[src, :], dy_v.at[dst, :]),
        )
        return [pltpu.make_async_copy(a, b, row_sem.at[parity, i]) for i, (a, b) in enumerate(pairs)]

    def wd_load(i):
        rows = pl.ds(i * ff_piece, ff_piece)
        return pltpu.make_async_copy(w_down.at[rows, :], w_d.at[rows, :], wd_sem.at[i])

    tiles = [(0, FIRST), (FIRST, piece - FIRST)] + [(c * piece, piece) for c in range(1, PIECES)]

    def wgu_loads(i):
        rows = pl.ds(*tiles[i])
        return [
            pltpu.make_async_copy(w.at[rows, :], w_gu.at[rows, pl.ds(j * ff, ff)], wgu_sem.at[i, j])
            for j, w in enumerate((w_gate, w_up))
        ]

    def x_load(step):
        return pltpu.make_async_copy(x.at[block_rows(step), :], w_gu.at[held(step), :], x_sem.at[step])

    def rs_copy(step, c, part=None):
        part = slice(None) if part is None else part
        return pltpu.make_async_remote_copy(
            src_ref=slots.at[step, c, :, part],
            dst_ref=slots.at[step + 1, c, :, part],
            send_sem=rs_send.at[step, c],
            recv_sem=rs_recv.at[step + 1, c],
            device_id={"tp": peer},
            device_id_type=MESH,
        )

    def columns(c):
        return pl.ds(pl.multiple_of(c * piece, piece), piece)

    def ag_copy(hop, c, own=False, into=None):
        place = dx.at[block_rows(hop + n - 1), columns(c)]
        return pltpu.make_async_remote_copy(
            src_ref=slots.at[n - 1, c] if own else place,
            dst_ref=place if into is None else into,
            send_sem=ag_send.at[hop, c],
            recv_sem=ag_recv.at[hop, c],
            device_id={"tp": peer},
            device_id_type=MESH,
        )

    def own_copy(c):
        return pltpu.make_async_copy(slots.at[n - 1, c], dx.at[block_rows(n - 1), columns(c)], own_sem.at[c])

    barrier = pltpu.get_barrier_semaphore()
    for other in (peer, behind):
        pl.semaphore_signal(barrier, inc=1, device_id={"tp": other}, device_id_type=MESH)
    for copy in row_loads(0):
        copy.start()
    for i in range(FF_PIECES):
        wd_load(i).start()
    pl.semaphore_wait(barrier, 2)

    def rs_step(step, _):
        loads = row_loads(step)
        for copy in loads[:2]:
            copy.wait()
        rows = held(step)
        for i in range(FF_PIECES):
            low, high = pl.ds(i * ff_piece, ff_piece), pl.ds(ff + i * ff_piece, ff_piece)
            g = d_gu[rows, low].astype(F32)
            value, back = jax.vjp(jax.nn.gelu, g)
            (slope,) = back(jnp.ones_like(g))
            term[:, low] = slope
            term[:, high] = value
            hid[rows, low] = (value * d_gu[rows, high].astype(F32)).astype(BF16)
        loads[2].wait()
        for i in range(FF_PIECES):
            @pl.when(step == 0)
            def _():
                wd_load(i).wait()
                for copy in wgu_loads(i):
                    copy.start()

            low, high = pl.ds(i * ff_piece, ff_piece), pl.ds(ff + i * ff_piece, ff_piece)
            d_hidden = dot_nt(dy_v[rows, :], w_d[low, :])
            d_gu[rows, low] = (d_hidden * d_gu[rows, high].astype(F32) * term[:, low]).astype(BF16)
            d_gu[rows, high] = (d_hidden * term[:, high]).astype(BF16)

        for i, (start, size) in enumerate(tiles):
            @pl.when(step == 0)
            def _():
                for copy in wgu_loads(i):
                    copy.wait()

            part = dot_nt(d_gu[rows, :], w_gu[start : start + size, :])

            @pl.when(step == 0)
            def _():
                c = start // piece
                cols = slice(start - c * piece, start - c * piece + size)
                slots[0, c, :, cols] = part.astype(BF16)
                rs_copy(0, c, cols).start()

            @pl.when(step > 0)
            def _():
                term[:, start : start + size] = part

        @pl.when(step < n - 1)
        def _():
            for copy in row_loads(step + 1):
                copy.start()

        @pl.when(step == n - 1)
        def _():
            for s in range(n):
                x_load(s).start()

        @pl.when(step > 0)
        def _():
            for c in range(PIECES):
                rs_copy(step - 1, c).wait_recv()
                total = slots[step, c].astype(F32) + term[:, c * piece : (c + 1) * piece]
                slots[step, c] = total.astype(BF16)

                @pl.when(step < n - 1)
                def _():
                    rs_copy(step, c).start()

                @pl.when(step == n - 1)
                def _():
                    ag_copy(0, c, own=True).start()
                    own_copy(c).start()

        return 0

    lax.fori_loop(0, n, rs_step, 0)

    down_tiles = ff // TILE
    up_tiles = width // TILE
    down_units = down_tiles * (width // ff)
    units = down_units + 2 * up_tiles

    def out_copy(unit):
        slot = lax.rem(unit, 2)
        return pltpu.make_async_copy(stage.at[slot], dw_gate.at[pl.ds(0, TILE), :], out_sem.at[slot])

    def work(unit):
        slot = lax.rem(unit, 2)

        @pl.when(unit >= 2)
        def _():
            out_copy(unit).wait()

        @pl.when(unit < down_units)
        def _():
            row = pl.ds(pl.multiple_of(lax.rem(unit, down_tiles) * TILE, TILE), TILE)
            col = pl.ds(pl.multiple_of(lax.div(unit, down_tiles) * ff, ff), ff)
            stage[slot] = dot_tn(hid[:, row], dy_v[:, col]).astype(BF16)
            pltpu.make_async_copy(stage.at[slot], dw_down.at[row, col], out_sem.at[slot]).start()

        @pl.when(unit == down_units)
        def _():
            for s in range(n):
                x_load(s).wait()

        @pl.when(unit >= down_units)
        def _():
            which = lax.div(unit - down_units, up_tiles)
            row = pl.ds(pl.multiple_of(lax.rem(unit - down_units, up_tiles) * TILE, TILE), TILE)
            col = pl.ds(pl.multiple_of(which * ff, ff), ff)
            stage[slot] = dot_tn(w_gu[pl.ds(0, tokens), row], d_gu[:, col]).astype(BF16)
            for i, out in enumerate((dw_gate, dw_up)):
                @pl.when(which == i)
                def _():
                    pltpu.make_async_copy(stage.at[slot], out.at[row, :], out_sem.at[slot]).start()

    per_turn = -(-units // turns)

    def ag_step(turn, _):
        for k in range(per_turn):
            @pl.when(turn * per_turn + k < units)
            def _():
                work(turn * per_turn + k)

        hop, c = lax.div(turn, PIECES), lax.rem(turn, PIECES)
        ag_copy(hop, c).wait_recv()

        @pl.when(turn < turns - 2 - PIECES)
        def _():
            ag_copy(hop + 1, c).start()

        @pl.when(turn == turns - 2 - PIECES)
        def _():
            ag_copy(hop + 1, c, into=early).start()

        @pl.when(turn == turns - 1 - PIECES)
        def _():
            ag_copy(hop + 1, c, into=late).start()

        return 0

    assert PIECES == 2 and FF_PIECES == 3 and n > 3 and width == 2 * ff and tokens <= width
    lax.fori_loop(0, turns, ag_step, 0)

    for unit in (units - 2, units - 1):
        out_copy(unit).wait()

    def sends(hop, _):
        for c in range(PIECES):
            rs_copy(hop, c).wait_send()

            @pl.when(hop * PIECES + c < turns)
            def _():
                ag_copy(hop, c).wait_send()

        return 0

    lax.fori_loop(0, n - 1, sends, 0)
    for c in range(PIECES):
        own_copy(c).wait()


def move(jobs, sems):
    loads = [pltpu.make_async_copy(a, v, sems.at[0, k]) for k, (a, v, _) in enumerate(jobs)]
    stores = [pltpu.make_async_copy(v, b, sems.at[1, k]) for k, (_, v, b) in enumerate(jobs)]
    for load in loads:
        load.start()
    for load, store in zip(loads, stores):
        load.wait()
        store.start()
    for store in stores:
        store.wait()


def outputs(n, dx_in, dw_down_in, early, late, dx, dw_down, wide, sems):
    block, piece = late.shape
    me = lax.axis_index("tp")
    ahead = 1 - 2 * lax.rem(lax.axis_index("dp"), 2)
    left, right = pl.ds(0, piece), pl.ds(piece, piece)
    jobs = []
    for i in range(n - 1):
        rows = pl.ds(pl.multiple_of(lax.rem(me + ahead - ahead * i + n, n) * block, block), block)
        here = pl.ds(i * block, block)
        if i < n - 3:
            jobs.append((dx_in.at[rows, :], wide.at[here, :], dx.at[rows, :]))
        else:
            jobs.append((dx_in.at[rows, left] if i == n - 3 else late, wide.at[here, left], dx.at[rows, left]))
        if i == n - 3:
            jobs.append((early, wide.at[here, right], dx.at[rows, right]))
    spot = (n - 1) * block
    for i in range(dw_down.shape[0] // TILE):
        rows = pl.ds(i * TILE, TILE)
        jobs.append((dw_down_in.at[rows, :], wide.at[pl.ds(spot + i * TILE, TILE), :], dw_down.at[rows, :]))
    move(jobs, sems)


def more_outputs(dw_gate_in, dw_up_in, after, dw_gate, dw_up, narrow, sems):
    del after
    step = 2 * TILE
    jobs = []
    for j, (a, b) in enumerate(((dw_gate_in, dw_gate), (dw_up_in, dw_up))):
        for i in range(b.shape[0] // step):
            rows = pl.ds(i * step, step)
            jobs.append((a.at[rows, :], narrow.at[j, rows, :], b.at[rows, :]))
    move(jobs, sems)


def solution(mesh):
    n, groups = mesh.shape["tp"], mesh.shape["dp"]

    def step(x, dy, gate, up, w_gate, w_up, w_down):
        tokens, width = x.shape
        ff = gate.shape[1]
        block, piece = tokens // n, width // PIECES
        hbm = pl.BlockSpec(memory_space=pl.ANY)
        results = [jax.ShapeDtypeStruct(a.shape, BF16) for a in (x, w_gate, w_up, w_down)]
        parts = pl.pallas_call(
            functools.partial(kernel, n),
            out_shape=results + [jax.ShapeDtypeStruct((block, piece), BF16)] * 2,
            in_specs=[hbm] * 7,
            out_specs=[hbm] * 6,
            scratch_shapes=[
                pltpu.VMEM((width, 2 * ff), BF16),
                pltpu.VMEM((ff, width), BF16),
                pltpu.VMEM((tokens, 2 * ff), BF16),
                pltpu.VMEM((tokens, ff), BF16),
                pltpu.VMEM((tokens, width), BF16),
                pltpu.VMEM((block, width), F32),
                pltpu.VMEM((n, PIECES, block, piece), BF16),
                pltpu.VMEM((2, TILE, ff), BF16),
                pltpu.SemaphoreType.DMA((2, 3)),
                pltpu.SemaphoreType.DMA((FF_PIECES,)),
                pltpu.SemaphoreType.DMA((PIECES + 1, 2)),
                pltpu.SemaphoreType.DMA((n,)),
                pltpu.SemaphoreType.DMA((2,)),
                pltpu.SemaphoreType.DMA((PIECES,)),
                pltpu.SemaphoreType.DMA((n, PIECES)),
                pltpu.SemaphoreType.DMA((n, PIECES)),
                pltpu.SemaphoreType.DMA((n, PIECES)),
                pltpu.SemaphoreType.DMA((n, PIECES)),
            ],
            compiler_params=pltpu.CompilerParams(
                collective_id=0, has_side_effects=True, vmem_limit_bytes=67_043_328
            ),
        )(x, dy, gate, up, w_gate, w_up, w_down)
        ring = [(d * n + i, d * n + (i + 1 - 2 * (d % 2)) % n) for d in range(groups) for i in range(n)]
        early, late = parts[4:]
        right = lax.ppermute(early, ("dp", "tp"), ring)
        last_left = lax.ppermute(late, ("dp", "tp"), ring)
        last_right = lax.ppermute(right, ("dp", "tp"), ring)
        cost = pl.CostEstimate(flops=2**33, bytes_accessed=2**24, transcendentals=0)
        dx, dw_down = pl.pallas_call(
            functools.partial(outputs, n),
            out_shape=[results[0], results[3]],
            in_specs=[hbm] * 4,
            out_specs=[hbm] * 2,
            scratch_shapes=[
                pltpu.VMEM(((n - 1) * block + ff, width), BF16),
                pltpu.SemaphoreType.DMA((2, n + ff // TILE)),
            ],
            cost_estimate=cost,
            compiler_params=pltpu.CompilerParams(has_side_effects=True),
        )(parts[0], parts[3], early, late)
        dw_gate, dw_up = pl.pallas_call(
            more_outputs,
            out_shape=results[1:3],
            in_specs=[hbm] * 3,
            out_specs=[hbm] * 2,
            scratch_shapes=[pltpu.VMEM((2, width, ff), BF16), pltpu.SemaphoreType.DMA((2, width // TILE))],
            cost_estimate=cost,
            compiler_params=pltpu.CompilerParams(has_side_effects=True),
        )(parts[1], parts[2], dw_down)
        me = lax.axis_index("tp")
        ahead = 1 - 2 * lax.rem(lax.axis_index("dp"), 2)
        end = lax.rem(me + 2 * ahead + n, n) * block
        dx = lax.dynamic_update_slice(dx, right, (lax.rem(me + 3 * ahead + n, n) * block, piece))
        dx = lax.dynamic_update_slice(dx, last_left, (end, 0))
        dx = lax.dynamic_update_slice(dx, last_right, (end, piece))
        return dx, dw_gate, dw_up, dw_down

    tokens, columns, rows = P("dp", None), P(None, "tp"), P("tp", None)
    return jax.shard_map(
        step,
        mesh=mesh,
        in_specs=(tokens, tokens, P("dp", "tp"), P("dp", "tp"), columns, columns, rows),
        out_specs=(tokens, P("dp", "tp"), P("dp", "tp"), P(("dp", "tp"), None)),
        check_vma=False,
    )
```

```python
import functools

import jax
import jax.numpy as jnp
from jax import lax
from jax.experimental import pallas as pl
from jax.experimental.pallas import tpu as pltpu
from jax.sharding import PartitionSpec as P

MESH = pl.DeviceIdType.MESH
F32 = jnp.float32
BF16 = jnp.bfloat16
PIECES = 2
FIRST = 256
FF_PIECES = 3
TILE = 384


def dot_nt(a, b):
    return lax.dot_general(a, b, (((1,), (1,)), ((), ())), preferred_element_type=F32)


def dot_tn(a, b):
    return lax.dot_general(a, b, (((0,), (0,)), ((), ())), preferred_element_type=F32)


def kernel(
    n,
    x, dy, gate, up, w_gate, w_up, w_down,
    dx, dw_gate, dw_up, dw_down, early, late,
    w_gu, w_d, d_gu, hid, dy_v, term, slots, stage,
    row_sem, wd_sem, wgu_sem, x_sem, out_sem, dx_sem, rs_send, rs_recv, ag_send, ag_recv,
):
    tokens, width = dy_v.shape
    ff = w_d.shape[0]
    block = tokens // n
    piece = width // PIECES
    ff_piece = ff // FF_PIECES
    me = lax.axis_index("tp")
    ahead = 1 - 2 * lax.rem(lax.axis_index("dp"), 2)
    peer = lax.rem(me + ahead + n, n)
    behind = lax.rem(me - ahead + n, n)
    hops = n - 2
    turns = (hops - 1) * PIECES + 1

    def block_rows(step):
        return pl.ds(pl.multiple_of(lax.rem(me - ahead * step + 2 * n, n) * block, block), block)

    def held(step):
        return pl.ds(pl.multiple_of(step * block, block), block)

    def row_loads(step):
        parity = lax.rem(step, 2)
        src, dst = block_rows(step), held(step)
        pairs = (
            (gate.at[src, :], d_gu.at[dst, pl.ds(0, ff)]),
            (up.at[src, :], d_gu.at[dst, pl.ds(ff, ff)]),
            (dy.at[src, :], dy_v.at[dst, :]),
        )
        return [pltpu.make_async_copy(a, b, row_sem.at[parity, i]) for i, (a, b) in enumerate(pairs)]

    def wd_load(i):
        rows = pl.ds(i * ff_piece, ff_piece)
        return pltpu.make_async_copy(w_down.at[rows, :], w_d.at[rows, :], wd_sem.at[i])

    tiles = [(0, FIRST), (FIRST, piece - FIRST)] + [(c * piece, piece) for c in range(1, PIECES)]

    def wgu_loads(i):
        rows = pl.ds(*tiles[i])
        return [
            pltpu.make_async_copy(w.at[rows, :], w_gu.at[rows, pl.ds(j * ff, ff)], wgu_sem.at[i, j])
            for j, w in enumerate((w_gate, w_up))
        ]

    def x_load(step):
        return pltpu.make_async_copy(x.at[block_rows(step), :], w_gu.at[held(step), :], x_sem.at[step])

    def rs_copy(step, c, part=None):
        part = slice(None) if part is None else part
        return pltpu.make_async_remote_copy(
            src_ref=slots.at[step, c, :, part],
            dst_ref=slots.at[step + 1, c, :, part],
            send_sem=rs_send.at[step, c],
            recv_sem=rs_recv.at[step + 1, c],
            device_id={"tp": peer},
            device_id_type=MESH,
        )

    def columns(c):
        return pl.ds(pl.multiple_of(c * piece, piece), piece)

    def ag_copy(hop, c, into=None):
        return pltpu.make_async_remote_copy(
            src_ref=slots.at[lax.rem(hop + n - 1, n + 1), c],
            dst_ref=slots.at[lax.rem(hop + n, n + 1), c] if into is None else into,
            send_sem=ag_send.at[hop, c],
            recv_sem=ag_recv.at[hop, c],
            device_id={"tp": peer},
            device_id_type=MESH,
        )

    def dx_copy(step, c):
        slot = lax.rem(step, n + 1)
        return pltpu.make_async_copy(slots.at[slot, c], dx.at[block_rows(step), columns(c)], dx_sem.at[slot, c])

    barrier = pltpu.get_barrier_semaphore()
    for other in (peer, behind):
        pl.semaphore_signal(barrier, inc=1, device_id={"tp": other}, device_id_type=MESH)
    for copy in row_loads(0):
        copy.start()
    for i in range(FF_PIECES):
        wd_load(i).start()
    pl.semaphore_wait(barrier, 2)

    def rs_step(step, _):
        loads = row_loads(step)
        for copy in loads[:2]:
            copy.wait()
        rows = held(step)
        for i in range(FF_PIECES):
            low, high = pl.ds(i * ff_piece, ff_piece), pl.ds(ff + i * ff_piece, ff_piece)
            g = d_gu[rows, low].astype(F32)
            value, back = jax.vjp(jax.nn.gelu, g)
            (slope,) = back(jnp.ones_like(g))
            term[:, low] = slope
            term[:, high] = value
            hid[rows, low] = (value * d_gu[rows, high].astype(F32)).astype(BF16)
        loads[2].wait()
        for i in range(FF_PIECES):
            @pl.when(step == 0)
            def _():
                wd_load(i).wait()
                for copy in wgu_loads(i):
                    copy.start()

            low, high = pl.ds(i * ff_piece, ff_piece), pl.ds(ff + i * ff_piece, ff_piece)
            d_hidden = dot_nt(dy_v[rows, :], w_d[low, :])
            d_gu[rows, low] = (d_hidden * d_gu[rows, high].astype(F32) * term[:, low]).astype(BF16)
            d_gu[rows, high] = (d_hidden * term[:, high]).astype(BF16)

        for i, (start, size) in enumerate(tiles):
            @pl.when(step == 0)
            def _():
                for copy in wgu_loads(i):
                    copy.wait()

            part = dot_nt(d_gu[rows, :], w_gu[start : start + size, :])

            @pl.when(step == 0)
            def _():
                c = start // piece
                cols = slice(start - c * piece, start - c * piece + size)
                slots[0, c, :, cols] = part.astype(BF16)
                rs_copy(0, c, cols).start()

            @pl.when(step > 0)
            def _():
                term[:, start : start + size] = part

        @pl.when(step < n - 1)
        def _():
            for copy in row_loads(step + 1):
                copy.start()

        @pl.when(step == n - 1)
        def _():
            for s in range(n):
                x_load(s).start()

        @pl.when(step > 0)
        def _():
            for c in range(PIECES):
                rs_copy(step - 1, c).wait_recv()
                rs_copy(step - 1, c).wait_send()
                total = slots[step, c].astype(F32) + term[:, c * piece : (c + 1) * piece]
                slots[step, c] = total.astype(BF16)

                @pl.when(step < n - 1)
                def _():
                    rs_copy(step, c).start()

                @pl.when(step == n - 1)
                def _():
                    ag_copy(0, c).start()
                    dx_copy(n - 1, c).start()

        return 0

    lax.fori_loop(0, n, rs_step, 0)

    down_tiles = ff // TILE
    up_tiles = width // TILE
    down_units = down_tiles * (width // ff)
    units = down_units + 2 * up_tiles

    def out_copy(unit):
        slot = lax.rem(unit, 2)
        return pltpu.make_async_copy(stage.at[slot], dw_gate.at[pl.ds(0, TILE), :], out_sem.at[slot])

    def work(unit):
        slot = lax.rem(unit, 2)

        @pl.when(unit >= 2)
        def _():
            out_copy(unit).wait()

        @pl.when(unit < down_units)
        def _():
            row = pl.ds(pl.multiple_of(lax.rem(unit, down_tiles) * TILE, TILE), TILE)
            col = pl.ds(pl.multiple_of(lax.div(unit, down_tiles) * ff, ff), ff)
            stage[slot] = dot_tn(hid[:, row], dy_v[:, col]).astype(BF16)
            pltpu.make_async_copy(stage.at[slot], dw_down.at[row, col], out_sem.at[slot]).start()

        @pl.when(unit == down_units)
        def _():
            for s in range(n):
                x_load(s).wait()

        @pl.when(unit >= down_units)
        def _():
            which = lax.div(unit - down_units, up_tiles)
            row = pl.ds(pl.multiple_of(lax.rem(unit - down_units, up_tiles) * TILE, TILE), TILE)
            col = pl.ds(pl.multiple_of(which * ff, ff), ff)
            stage[slot] = dot_tn(w_gu[pl.ds(0, tokens), row], d_gu[:, col]).astype(BF16)
            for i, out in enumerate((dw_gate, dw_up)):
                @pl.when(which == i)
                def _():
                    pltpu.make_async_copy(stage.at[slot], out.at[row, :], out_sem.at[slot]).start()

    per_turn = -(-units // turns)

    def ag_step(turn, _):
        for k in range(per_turn):
            @pl.when(turn * per_turn + k < units)
            def _():
                work(turn * per_turn + k)

        hop, c = lax.div(turn, PIECES), lax.rem(turn, PIECES)
        ag_copy(hop, c).wait_recv()

        @pl.when(turn < turns - 2)
        def _():
            dx_copy(hop + n, c).start()

        @pl.when(turn < turns - 2 - PIECES)
        def _():
            ag_copy(hop + 1, c).start()

        @pl.when(turn == turns - 2 - PIECES)
        def _():
            ag_copy(hop + 1, c, into=early).start()

        @pl.when(turn == turns - 1 - PIECES)
        def _():
            ag_copy(hop + 1, c, into=late).start()

        return 0

    assert PIECES == 2 and FF_PIECES == 3 and n > 3 and width == 2 * ff and tokens <= width
    lax.fori_loop(0, turns, ag_step, 0)

    for unit in (units - 2, units - 1):
        out_copy(unit).wait()

    def sends(hop, _):
        for c in range(PIECES):
            @pl.when(hop * PIECES + c < turns)
            def _():
                ag_copy(hop, c).wait_send()

            @pl.when(hop * PIECES + c < turns - 2)
            def _():
                dx_copy(hop + n, c).wait()

        return 0

    lax.fori_loop(0, n - 1, sends, 0)
    for c in range(PIECES):
        dx_copy(n - 1, c).wait()


def move(jobs, sems):
    loads = [pltpu.make_async_copy(a, v, sems.at[0, k]) for k, (a, v, _) in enumerate(jobs)]
    stores = [pltpu.make_async_copy(v, b, sems.at[1, k]) for k, (_, v, b) in enumerate(jobs)]
    for load in loads:
        load.start()
    for load, store in zip(loads, stores):
        load.wait()
        store.start()
    for store in stores:
        store.wait()


def outputs(n, dx_in, dw_down_in, early, late, dx, dw_down, wide, sems):
    block, piece = late.shape
    me = lax.axis_index("tp")
    ahead = 1 - 2 * lax.rem(lax.axis_index("dp"), 2)
    left, right = pl.ds(0, piece), pl.ds(piece, piece)
    jobs = []
    for i in range(n - 1):
        rows = pl.ds(pl.multiple_of(lax.rem(me + ahead - ahead * i + n, n) * block, block), block)
        here = pl.ds(i * block, block)
        if i < n - 3:
            jobs.append((dx_in.at[rows, :], wide.at[here, :], dx.at[rows, :]))
        else:
            jobs.append((dx_in.at[rows, left] if i == n - 3 else late, wide.at[here, left], dx.at[rows, left]))
        if i == n - 3:
            jobs.append((early, wide.at[here, right], dx.at[rows, right]))
    spot = (n - 1) * block
    for i in range(dw_down.shape[0] // TILE):
        rows = pl.ds(i * TILE, TILE)
        jobs.append((dw_down_in.at[rows, :], wide.at[pl.ds(spot + i * TILE, TILE), :], dw_down.at[rows, :]))
    move(jobs, sems)


def more_outputs(dw_gate_in, dw_up_in, after, dw_gate, dw_up, narrow, sems):
    del after
    step = 2 * TILE
    jobs = []
    for j, (a, b) in enumerate(((dw_gate_in, dw_gate), (dw_up_in, dw_up))):
        for i in range(b.shape[0] // step):
            rows = pl.ds(i * step, step)
            jobs.append((a.at[rows, :], narrow.at[j, rows, :], b.at[rows, :]))
    move(jobs, sems)


def solution(mesh):
    n, groups = mesh.shape["tp"], mesh.shape["dp"]

    def step(x, dy, gate, up, w_gate, w_up, w_down):
        tokens, width = x.shape
        ff = gate.shape[1]
        block, piece = tokens // n, width // PIECES
        hbm = pl.BlockSpec(memory_space=pl.ANY)
        results = [jax.ShapeDtypeStruct(a.shape, BF16) for a in (x, w_gate, w_up, w_down)]
        parts = pl.pallas_call(
            functools.partial(kernel, n),
            out_shape=results + [jax.ShapeDtypeStruct((block, piece), BF16)] * 2,
            in_specs=[hbm] * 7,
            out_specs=[hbm] * 6,
            scratch_shapes=[
                pltpu.VMEM((width, 2 * ff), BF16),
                pltpu.VMEM((ff, width), BF16),
                pltpu.VMEM((tokens, 2 * ff), BF16),
                pltpu.VMEM((tokens, ff), BF16),
                pltpu.VMEM((tokens, width), BF16),
                pltpu.VMEM((block, width), F32),
                pltpu.VMEM((n + 1, PIECES, block, piece), BF16),
                pltpu.VMEM((2, TILE, ff), BF16),
                pltpu.SemaphoreType.DMA((2, 3)),
                pltpu.SemaphoreType.DMA((FF_PIECES,)),
                pltpu.SemaphoreType.DMA((PIECES + 1, 2)),
                pltpu.SemaphoreType.DMA((n,)),
                pltpu.SemaphoreType.DMA((2,)),
                pltpu.SemaphoreType.DMA((n + 1, PIECES)),
                pltpu.SemaphoreType.DMA((n, PIECES)),
                pltpu.SemaphoreType.DMA((n, PIECES)),
                pltpu.SemaphoreType.DMA((n, PIECES)),
                pltpu.SemaphoreType.DMA((n, PIECES)),
            ],
            compiler_params=pltpu.CompilerParams(
                collective_id=0, has_side_effects=True, vmem_limit_bytes=67_043_328
            ),
        )(x, dy, gate, up, w_gate, w_up, w_down)
        ring = [(d * n + i, d * n + (i + 1 - 2 * (d % 2)) % n) for d in range(groups) for i in range(n)]
        early, late = parts[4:]
        right = lax.ppermute(early, ("dp", "tp"), ring)
        last_left = lax.ppermute(late, ("dp", "tp"), ring)
        last_right = lax.ppermute(right, ("dp", "tp"), ring)
        cost = pl.CostEstimate(flops=2**33, bytes_accessed=2**24, transcendentals=0)
        dx, dw_down = pl.pallas_call(
            functools.partial(outputs, n),
            out_shape=[results[0], results[3]],
            in_specs=[hbm] * 4,
            out_specs=[hbm] * 2,
            scratch_shapes=[
                pltpu.VMEM(((n - 1) * block + ff, width), BF16),
                pltpu.SemaphoreType.DMA((2, n + ff // TILE)),
            ],
            cost_estimate=cost,
            compiler_params=pltpu.CompilerParams(has_side_effects=True),
        )(parts[0], parts[3], early, late)
        dw_gate, dw_up = pl.pallas_call(
            more_outputs,
            out_shape=results[1:3],
            in_specs=[hbm] * 3,
            out_specs=[hbm] * 2,
            scratch_shapes=[pltpu.VMEM((2, width, ff), BF16), pltpu.SemaphoreType.DMA((2, width // TILE))],
            cost_estimate=cost,
            compiler_params=pltpu.CompilerParams(has_side_effects=True),
        )(parts[1], parts[2], dw_down)
        me = lax.axis_index("tp")
        ahead = 1 - 2 * lax.rem(lax.axis_index("dp"), 2)
        end = lax.rem(me + 2 * ahead + n, n) * block
        dx = lax.dynamic_update_slice(dx, right, (lax.rem(me + 3 * ahead + n, n) * block, piece))
        dx = lax.dynamic_update_slice(dx, last_left, (end, 0))
        dx = lax.dynamic_update_slice(dx, last_right, (end, piece))
        return dx, dw_gate, dw_up, dw_down

    tokens, columns, rows = P("dp", None), P(None, "tp"), P("tp", None)
    return jax.shard_map(
        step,
        mesh=mesh,
        in_specs=(tokens, tokens, P("dp", "tp"), P("dp", "tp"), columns, columns, rows),
        out_specs=(tokens, P("dp", "tp"), P("dp", "tp"), P(("dp", "tp"), None)),
        check_vma=False,
    )
```
